128 devices in a mesh: quant: 16 (over y, x_lo, core), head: 8 (over x_hi, z).
Axes of the slice: x: 4 (x_hi: 2, x_lo: 2; x = x_hi * 2 + x_lo), y: 4, z: 4, core: 2. Of those that a mesh axis runs over, the one named last changes fastest.
Arguments:
- tokens: bfloat16 [24576, 8192], P('quant', 'head'), may hold values from -6 to 6
- packed_words: int32 [2048, 2048], P('head', 'quant'), may hold values from 0 to 65535
- scales: float32 [64, 2048], replicated, may hold values from 0.0008 to 0.008
- act_order: int32 [8192], replicated, may hold values from 0 to 8191, each once
- head_map: int32 [8], replicated, may hold values from 0 to 7, each once
Outputs:
- keys_out: bfloat16 [24576, 1024], P('quant', 'head')
- values_out: bfloat16 [24576, 1024], P('quant', 'head')
The draws below stay inside these ranges and needn't reach their ends.
Inputs may be any that keep to these rules, and one draw needn't show every extreme that they name: Bits 4k to 4k + 3 of packed_words[p, c] hold the code of permuted row 4p + k, for k < 4; the other bits are zero. `act_order`: a permutation of the input features. `head_map`: a permutation of the key-value heads.
All inputs are finite; a program needn't handle non-finite values.
Results may differ from the reference program's by a relative error of at most 0.0049.
Values may be sent and summed in bfloat16 or wider, within the bound.
No kernel may reach another device: no remote copies, remote signals or barrier semaphores. Data moves between devices by JAX's collectives and lax.ppermute only.
A program may use at most 128 MiB of HBM per device.

```python
import math
import jax
import jax.numpy as jnp

D = 8192
KV = 8
HD = 128
G = 128
TOKENS = 24576


def touch_ends(values, rng, low, top_value):
    dims = values.shape
    index_at = [jax.random.randint(jax.random.fold_in(rng, axis), (), 0, dims[axis]) for axis in range(len(dims))]
    values = values.at[tuple(index_at)].set(low)
    longest = dims.index(max(dims))
    index_at[longest] = (index_at[longest] + 1) % dims[longest]
    return values.at[tuple(index_at)].set(top_value)


def level_of(key, dims, cuts, smallest, high):
    def one(axis_at, blocks):
        steps = jax.random.uniform(jax.random.fold_in(jax.random.fold_in(key, 6), axis_at), (blocks,), jnp.float32, smallest / len(cuts), high / len(cuts))
        return jnp.repeat(jnp.exp(steps), dims[axis_at] // blocks).reshape((-1,) + (1,) * (len(dims) - axis_at - 1))

    loudness = one(*cuts[0])
    for cut in cuts[1:]:
        loudness = loudness * one(*cut)
    return loudness


def normal_values(rng, shape, scale, most, split=(), held_as=jnp.bfloat16):
    result = jax.random.normal(rng, shape, jnp.float32) * scale
    if len(split) > 0:
        result = level_of(rng, shape, split, -0.22, 0.18) * result
    return jnp.clip(result, min=-most, max=most).astype(held_as)


def setup_inputs(seed: int = 0) -> dict:
    key_list = jax.random.split(jax.random.key(seed), 6)
    return {
        "tokens": normal_values(key_list[0], (TOKENS, D), 1.0, 6.0, ((0, 16), (1, 8))),
        "packed_words": touch_ends(jax.random.randint(key_list[1], (D // 4, 2 * KV * HD), 0, 65536), jax.random.fold_in(key_list[1], 1), 0, 65535).astype(jnp.int32),
        "scales": jnp.clip(jnp.exp(jax.random.uniform(key_list[2], (D // G, 2 * KV * HD), jnp.float32, math.log(0.0008), math.log(0.008))), 0.0008, 0.008),
        "act_order": jax.random.permutation(key_list[3], D).astype(jnp.int32),
        "head_map": jax.random.permutation(key_list[4], KV).astype(jnp.int32),
    }


def reference(tokens, packed_words, scales, act_order, head_map):
    cols = 2 * KV * HD
    pieces = [jnp.bitwise_and(jnp.right_shift(packed_words, 4 * k), 15) for k in range(4)]
    codes = jnp.stack(pieces, axis=1).reshape(D, cols)
    scaled = (codes - 8).astype(jnp.float32).reshape(D // G, G, cols) * scales[:, None, :]
    dequant = scaled.reshape(D, cols).astype(jnp.bfloat16)
    weight = jnp.zeros((D, cols), jnp.bfloat16).at[act_order].set(dequant)
    product = jnp.dot(tokens, weight, preferred_element_type=jnp.float32)
    blocks = product.reshape(product.shape[0], 2, KV, HD)
    chosen = jnp.take(blocks, head_map, axis=2)
    keys_out = chosen[:, 0].reshape(product.shape[0], KV * HD).astype(jnp.bfloat16)
    values_out = chosen[:, 1].reshape(product.shape[0], KV * HD).astype(jnp.bfloat16)
    return keys_out, values_out
```

```python
import functools
import jax
import jax.numpy as jnp
from jax import lax
from jax.experimental import pallas as pl
from jax.experimental.pallas import tpu as pltpu
from jax.sharding import PartitionSpec as P


KV = 8
HD = 128
G = 128
CHUNKS = (512, 512, 512)


def position():
    head = lax.axis_index("head")
    quant = lax.axis_index("quant")
    return head // 4, head % 4, quant // 4, (quant // 2) % 2, quant % 2


def over_head(value, dx, dz):
    pairs = [
        (xh * 4 + z, (xh ^ dx) * 4 + (z + dz) % 4) for xh in range(2) for z in range(4)
    ]
    return lax.ppermute(value, "head", pairs)


def over_quant(value, dy, dx, dc):
    pairs = [
        (y * 4 + x * 2 + c, (y + dy) % 4 * 4 + (x ^ dx) * 2 + (c ^ dc))
        for y in range(4)
        for x in range(2)
        for c in range(2)
    ]
    return lax.ppermute(value, "quant", pairs)


def cost(flops, moved):
    return pl.CostEstimate(flops=flops, bytes_accessed=moved, transcendentals=0)


def vmem(count):
    return [pl.BlockSpec(memory_space=pltpu.VMEM)] * count


def dequant_kernel(words_ref, scales_ref, out_ref):
    words = words_ref.shape[0]
    groups = words * 4 // G
    head = lax.axis_index("head")
    quant = lax.axis_index("quant")
    scale = scales_ref[
        pl.ds(pl.multiple_of(head * groups, groups), groups),
        pl.ds(pl.multiple_of(quant * HD, HD), HD),
    ]
    spread = jnp.broadcast_to(scale[:, None, :], (groups, words // groups, HD)).reshape(
        words, HD
    )
    held = words_ref[...]
    for k in range(4):
        codes = jnp.bitwise_and(jnp.right_shift(held, 4 * k), 15)
        out_ref[k * words : (k + 1) * words, :] = (
            (codes - 8).astype(jnp.float32) * spread
        ).astype(jnp.bfloat16)


def dequantized(words, scales):
    rows = words.shape[0] * 4
    return pl.pallas_call(
        dequant_kernel,
        out_shape=jax.ShapeDtypeStruct((rows, HD), jnp.bfloat16),
        in_specs=vmem(2),
        out_specs=vmem(1)[0],
        name="dequant",
        cost_estimate=cost(2_000_000, 1_000_000),
    )(words, scales)


def unpermute_kernel(steps, order_ref, *refs):
    blocks, out_ref, total = refs[:-2], refs[-2], refs[-1]
    rows = out_ref.shape[0]
    head = lax.axis_index("head")
    x_hi, z = head // 4, head % 4
    for at, (dx, dz) in enumerate(steps):
        source = jnp.bitwise_xor(x_hi, dx) * 4 + (z - dz + 4) % 4
        order = order_ref[source]
        block = blocks[at][...]
        for start in range(0, rows, 256):
            feature = lax.broadcasted_iota(jnp.int32, (256, order.shape[1]), 0) + (
                head * rows + start
            )
            picked = jnp.where(feature == order, 1.0, 0.0).astype(jnp.bfloat16)
            part = jnp.dot(picked, block, preferred_element_type=jnp.float32)
            if at == 0:
                total[start : start + 256, :] = part
            else:
                total[start : start + 256, :] += part
    out_ref[...] = total[...].astype(jnp.bfloat16)


def unpermuted(order, steps, blocks):
    rows = blocks[0].shape[0]
    return pl.pallas_call(
        functools.partial(unpermute_kernel, steps),
        out_shape=jax.ShapeDtypeStruct((rows, HD), jnp.bfloat16),
        in_specs=vmem(1 + len(blocks)),
        out_specs=vmem(1)[0],
        scratch_shapes=[pltpu.VMEM((rows, HD), jnp.float32)],
        name="unpermute",
        cost_estimate=cost(2 * rows * rows * 8 * HD, 3_000_000),
    )(order, *blocks)


def message_head(map_ref, relative, dz):
    head = lax.axis_index("head")
    x_hi, z = head // 4, head % 4
    return map_ref[jnp.bitwise_xor(x_hi, relative) * 4 + (z + dz) % 4]


def messages(map_ref, x_ref, weight_ref, outs):
    rows = x_ref.shape[0]
    tile = 256
    for m in range(8):
        served = message_head(map_ref, m // 4, m % 4)
        weight = jnp.concatenate([weight_ref[served], weight_ref[8 + served]], axis=1)
        for start in range(0, rows, tile):
            outs[m][start : start + tile, :] = jnp.dot(
                x_ref[start : start + tile, :], weight, preferred_element_type=jnp.float32
            ).astype(jnp.bfloat16)


def first_kernel(places, map_ref, x_ref, *refs):
    blocks = refs[: len(places)]
    weight_ref = refs[len(places)]
    outs = refs[len(places) + 1 :]
    quant = lax.axis_index("quant")
    y, x_lo, core = quant // 4, (quant // 2) % 2, quant % 2
    for block, (dy, dx, dc) in zip(blocks, places):
        source = (
            (y - dy + 4) % 4 * 4
            + jnp.bitwise_xor(x_lo, dx) * 2
            + jnp.bitwise_xor(core, dc)
        )
        weight_ref[source] = block[...]
    messages(map_ref, x_ref, weight_ref, outs)


def later_kernel(map_ref, x_ref, weight_ref, *outs):
    messages(map_ref, x_ref, weight_ref, outs)


def products(tokens, head_map, start, rows, weight, places, blocks):
    depth = tokens.shape[1]
    outs = [jax.ShapeDtypeStruct((rows, 2 * HD), jnp.bfloat16)] * 8
    specs = [
        pl.BlockSpec(memory_space=pltpu.SMEM),
        pl.BlockSpec((rows, depth), lambda i: (start // rows, 0)),
    ]
    whole = [pl.BlockSpec((rows, 2 * HD), lambda i: (0, 0))] * 8
    estimate = cost(2 * rows * depth * 16 * HD, 8_000_000)
    if weight is None:
        shape = (16, depth, HD)
        got = pl.pallas_call(
            functools.partial(first_kernel, places),
            grid=(1,),
            out_shape=[jax.ShapeDtypeStruct(shape, jnp.bfloat16)] + outs,
            in_specs=specs + [pl.BlockSpec((depth, HD), lambda i: (0, 0))] * len(blocks),
            out_specs=[pl.BlockSpec(shape, lambda i: (0, 0, 0))] + whole,
            name="products_first",
            cost_estimate=estimate,
        )(head_map, tokens, *blocks)
        return got[0], got[1:]
    got = pl.pallas_call(
        later_kernel,
        grid=(1,),
        out_shape=outs,
        in_specs=specs + [pl.BlockSpec(weight.shape, lambda i: (0, 0, 0))],
        out_specs=whole,
        name="products_later",
        cost_estimate=estimate,
    )(head_map, tokens, weight)
    return weight, got


def added(*terms):
    total = terms[0].astype(jnp.float32)
    for term in terms[1:]:
        total = total + term.astype(jnp.float32)
    return total


def narrow(value):
    return value.astype(jnp.bfloat16)


def z_then_x(part):
    keep, send = part[:4], part[4:]
    relay_up = over_head(keep[2], 0, 1)
    relay_down = over_head(send[2], 0, -1)
    direct_up = over_head(send[1], 0, 1)
    direct_down = over_head(keep[3], 0, -1)
    summed_up = over_head(narrow(added(keep[1], relay_up)), 0, 1)
    summed_down = over_head(narrow(added(send[3], relay_down)), 0, -1)
    across = over_head(narrow(added(send[0], direct_up, summed_down)), 1, 0)
    return narrow(added(keep[0], summed_up, direct_down, across))


def body(tokens, packed_words, scales, act_order, head_map):
    depth = tokens.shape[1]
    words = packed_words.shape[0]
    owned = dequantized(packed_words, scales)
    order = jnp.transpose(act_order.reshape(-1, words, 4), (0, 2, 1)).reshape(-1, 1, 4 * words)
    steps = [(0, 0)] + [(dx, dz) for dx in range(2) for dz in range(4) if dx or dz]
    rows = [owned] + [over_head(owned, dx, dz) for dx, dz in steps[1:]]
    natural = unpermuted(order, steps, rows)
    near = [(0, 0, 0)] + [(dy, dx, 0) for dy in range(4) for dx in range(2) if dy or dx]
    blocks = [natural] + [over_quant(natural, *step) for step in near[1:]]
    places = near + [(dy, dx, 1) for dy, dx, _ in near]
    blocks = blocks + [over_quant(block, 0, 0, 1) for block in blocks]
    weight = None
    start = 0
    done = []
    for count in CHUNKS:
        weight, part = products(tokens, head_map, start, count, weight, places, blocks)
        done.append(z_then_x(part))
        start += count
    keys_out = jnp.concatenate([block[:, :HD] for block in done], axis=0)
    values_out = jnp.concatenate([block[:, HD:] for block in done], axis=0)
    return keys_out, values_out


def solution(mesh):
    placed = (P("quant", "head"), P("head", "quant"), P(), P(), P())
    return jax.shard_map(
        body,
        mesh=mesh,
        in_specs=placed,
        out_specs=(P("quant", "head"), P("quant", "head")),
        check_vma=False,
    )
```

```python
import functools
import jax
import jax.numpy as jnp
from jax import lax
from jax.experimental import pallas as pl
from jax.experimental.pallas import tpu as pltpu
from jax.sharding import PartitionSpec as P


KV = 8
HD = 128
G = 128
CHUNKS = (512, 512, 512)
CAP = 192


def over_head(value, dx, dz):
    pairs = [
        (xh * 4 + z, (xh ^ dx) * 4 + (z + dz) % 4) for xh in range(2) for z in range(4)
    ]
    return lax.ppermute(value, "head", pairs)


def over_quant(value, dy, dx, dc):
    pairs = [
        (y * 4 + x * 2 + c, (y + dy) % 4 * 4 + (x ^ dx) * 2 + (c ^ dc))
        for y in range(4)
        for x in range(2)
        for c in range(2)
    ]
    return lax.ppermute(value, "quant", pairs)


def cost(flops, moved):
    return pl.CostEstimate(flops=flops, bytes_accessed=moved, transcendentals=0)


def vmem(count):
    return [pl.BlockSpec(memory_space=pltpu.VMEM)] * count


def dequantize(words_ref, scales_ref, owned):
    words = words_ref.shape[0]
    groups = words * 4 // G
    head = lax.axis_index("head")
    quant = lax.axis_index("quant")
    scale = scales_ref[
        pl.ds(pl.multiple_of(head * groups, groups), groups),
        pl.ds(pl.multiple_of(quant * HD, HD), HD),
    ]
    spread = jnp.broadcast_to(scale[:, None, :], (groups, words // groups, HD)).reshape(
        words, HD
    )
    held = words_ref[...]
    for k in range(4):
        codes = jnp.bitwise_and(jnp.right_shift(held, 4 * k), 15)
        owned[pl.ds(k, words, stride=4), :] = (codes - 8).astype(jnp.float32) * spread


def one_hot(rows, numbers, first=0):
    at = lax.broadcasted_iota(jnp.int32, (rows, numbers.shape[1]), 0) + first
    return jnp.where(at == numbers, 1.0, 0.0).astype(jnp.bfloat16)


def in_lanes(block):
    return jnp.concatenate([block[s : s + 1, :] for s in range(block.shape[0])], axis=1)


def pack_kernel(steps, words_ref, scales_ref, order_ref, *refs):
    packed, owned_ref, most_ref, owned, rank_ref = (
        refs[: len(steps)],
        refs[-4],
        refs[-3],
        refs[-2],
        refs[-1],
    )
    dequantize(words_ref, scales_ref, owned)
    rows = owned.shape[0]
    lines = rows // HD
    parts = rank_ref.shape[0]
    head = lax.axis_index("head")
    x_hi, z = head // 4, head % 4
    block = owned[...].astype(jnp.bfloat16)
    owned_ref[...] = block
    fullest = jnp.zeros((lines, HD), jnp.float32)
    for source in range(parts):
        to = order_ref[source * lines : (source + 1) * lines, :] // rows
        for d in range(parts):
            count = jnp.sum(jnp.where(to == d, 1.0, 0.0))
            fullest = jnp.maximum(fullest, count)
    most_ref[...] = fullest.astype(jnp.int32)
    mine = order_ref[pl.ds(pl.multiple_of(head * lines, lines), lines), :]
    goes = mine // rows
    upto = jnp.where(
        lax.broadcasted_iota(jnp.int32, (HD, HD), 0)
        <= lax.broadcasted_iota(jnp.int32, (HD, HD), 1),
        1.0,
        0.0,
    ).astype(jnp.bfloat16)
    for d in range(parts):
        held = jnp.where(goes == d, 1.0, 0.0)
        within = jnp.dot(held.astype(jnp.bfloat16), upto, preferred_element_type=jnp.float32)
        before = jnp.zeros((1, 1), jnp.float32)
        ranks = []
        for s in range(lines):
            ranks.append(within[s : s + 1, :] + before)
            before = before + within[s : s + 1, HD - 1 : HD]
        rank = jnp.concatenate(ranks, axis=0)
        rank_ref[d] = jnp.where(goes == d, rank - 1.0, -1.0).astype(jnp.int32)
    feature = mine % rows
    halves = jnp.concatenate(
        [in_lanes(feature // 32), in_lanes(feature % 32)], axis=0
    ).astype(jnp.float32)
    halves = jnp.concatenate([halves] + [jnp.zeros_like(halves)] * 3, axis=0)
    halves = halves.astype(jnp.bfloat16)
    for at, (dx, dz) in enumerate(steps):
        target = jnp.bitwise_xor(x_hi, dx) * 4 + (z + dz) % 4
        picked = one_hot(CAP, in_lanes(rank_ref[target]))
        packed[at][:CAP, :] = jnp.dot(
            picked, block, preferred_element_type=jnp.float32
        ).astype(jnp.bfloat16)
        numbers = lax.dot_general(
            halves, picked, (((1,), (1,)), ((), ())), preferred_element_type=jnp.float32
        )
        wide = jnp.concatenate([numbers, jnp.zeros((8, 2 * HD - CAP), jnp.float32)], axis=1)
        packed[at][CAP:, :] = jnp.concatenate([wide[:, :HD], wide[:, HD:]], axis=0).astype(
            jnp.bfloat16
        )


def packed_rows(words, scales, order, steps):
    rows = words.shape[0] * 4
    return pl.pallas_call(
        functools.partial(pack_kernel, steps),
        out_shape=[jax.ShapeDtypeStruct((CAP + 16, HD), jnp.bfloat16)] * len(steps)
        + [
            jax.ShapeDtypeStruct((rows, HD), jnp.bfloat16),
            jax.ShapeDtypeStruct((8, HD), jnp.int32),
        ],
        in_specs=vmem(3),
        out_specs=vmem(len(steps) + 2),
        scratch_shapes=[
            pltpu.VMEM((rows, HD), jnp.float32),
            pltpu.VMEM((len(steps), rows // HD, HD), jnp.int32),
        ],
        name="pack",
        cost_estimate=cost(1_000_000_000, 3_000_000),
    )(words, scales, order)


def unpack_kernel(*refs):
    packed, out_ref = refs[:-1], refs[-1]
    rows = out_ref.shape[0]
    total = None
    for ref in packed:
        tail = ref[CAP:, :].astype(jnp.float32).astype(jnp.int32)
        number = jnp.concatenate(
            [tail[0:1, :] * 32 + tail[1:2, :], tail[8:9, :] * 32 + tail[9:10, :]], axis=1
        )
        part = jnp.dot(
            one_hot(rows, number[:, :CAP]), ref[:CAP, :], preferred_element_type=jnp.float32
        )
        total = part if total is None else total + part
    out_ref[...] = total.astype(jnp.bfloat16)


def unpacked(rows, blocks):
    return pl.pallas_call(
        unpack_kernel,
        out_shape=jax.ShapeDtypeStruct((rows, HD), jnp.bfloat16),
        in_specs=vmem(len(blocks)),
        out_specs=vmem(1)[0],
        name="unpack",
        cost_estimate=cost(1_000_000_000, 1_000_000),
    )(*blocks)


def pick_kernel(order_ref, every_ref, out_ref):
    rows = out_ref.shape[0]
    lines = rows // HD
    head = lax.axis_index("head")
    total = None
    for source in range(every_ref.shape[0]):
        order = in_lanes(order_ref[source * lines : (source + 1) * lines, :])
        part = jnp.dot(
            one_hot(rows, order, head * rows),
            every_ref[source],
            preferred_element_type=jnp.float32,
        )
        total = part if total is None else total + part
    out_ref[...] = total.astype(jnp.bfloat16)


def from_all_rows(order, owned):
    parts = lax.axis_size("head")
    every = lax.all_to_all(
        jnp.broadcast_to(owned[None], (parts, *owned.shape)), "head", 0, 0, tiled=True
    )
    return pl.pallas_call(
        pick_kernel,
        out_shape=jax.ShapeDtypeStruct(owned.shape, jnp.bfloat16),
        in_specs=vmem(2),
        out_specs=vmem(1)[0],
        name="pick",
    )(order, every)


def message_head(map_ref, relative, dz):
    head = lax.axis_index("head")
    x_hi, z = head // 4, head % 4
    return map_ref[jnp.bitwise_xor(x_hi, relative) * 4 + (z + dz) % 4]


def messages(map_ref, x_ref, weight_ref, outs):
    rows = x_ref.shape[0]
    tile = 256
    for m in range(8):
        served = message_head(map_ref, m // 4, m % 4)
        weight = jnp.concatenate([weight_ref[served], weight_ref[8 + served]], axis=1)
        for start in range(0, rows, tile):
            outs[m][start : start + tile, :] = jnp.dot(
                x_ref[start : start + tile, :], weight, preferred_element_type=jnp.float32
            ).astype(jnp.bfloat16)


def first_kernel(places, map_ref, x_ref, *refs):
    blocks = refs[: len(places)]
    weight_ref = refs[len(places)]
    outs = refs[len(places) + 1 :]
    quant = lax.axis_index("quant")
    y, x_lo, core = quant // 4, (quant // 2) % 2, quant % 2
    for block, (dy, dx, dc) in zip(blocks, places):
        source = (
            (y - dy + 4) % 4 * 4
            + jnp.bitwise_xor(x_lo, dx) * 2
            + jnp.bitwise_xor(core, dc)
        )
        weight_ref[source] = block[...]
    messages(map_ref, x_ref, weight_ref, outs)


def later_kernel(map_ref, x_ref, weight_ref, *outs):
    messages(map_ref, x_ref, weight_ref, outs)


def products(tokens, head_map, start, rows, weight, places, blocks):
    depth = tokens.shape[1]
    outs = [jax.ShapeDtypeStruct((rows, 2 * HD), jnp.bfloat16)] * 8
    specs = [
        pl.BlockSpec(memory_space=pltpu.SMEM),
        pl.BlockSpec((rows, depth), lambda i: (start // rows, 0)),
    ]
    whole = [pl.BlockSpec((rows, 2 * HD), lambda i: (0, 0))] * 8
    estimate = cost(2 * rows * depth * 16 * HD, 8_000_000)
    if weight is None:
        shape = (16, depth, HD)
        got = pl.pallas_call(
            functools.partial(first_kernel, places),
            grid=(1,),
            out_shape=[jax.ShapeDtypeStruct(shape, jnp.bfloat16)] + outs,
            in_specs=specs + [pl.BlockSpec((depth, HD), lambda i: (0, 0))] * len(blocks),
            out_specs=[pl.BlockSpec(shape, lambda i: (0, 0, 0))] + whole,
            name="products_first",
            cost_estimate=estimate,
        )(head_map, tokens, *blocks)
        return got[0], got[1:]
    got = pl.pallas_call(
        later_kernel,
        grid=(1,),
        out_shape=outs,
        in_specs=specs + [pl.BlockSpec(weight.shape, lambda i: (0, 0, 0))],
        out_specs=whole,
        name="products_later",
        cost_estimate=estimate,
    )(head_map, tokens, weight)
    return weight, got


def added(*terms):
    total = terms[0].astype(jnp.float32)
    for term in terms[1:]:
        total = total + term.astype(jnp.float32)
    return total


def narrow(value):
    return value.astype(jnp.bfloat16)


def z_then_x(part):
    keep, send = part[:4], part[4:]
    relay_up = over_head(keep[2], 0, 1)
    relay_down = over_head(send[2], 0, -1)
    direct_up = over_head(send[1], 0, 1)
    direct_down = over_head(keep[3], 0, -1)
    summed_up = over_head(narrow(added(keep[1], relay_up)), 0, 1)
    summed_down = over_head(narrow(added(send[3], relay_down)), 0, -1)
    across = over_head(narrow(added(send[0], direct_up, summed_down)), 1, 0)
    return narrow(added(keep[0], summed_up, direct_down, across))


def body(tokens, packed_words, scales, act_order, head_map):
    depth = tokens.shape[1]
    steps = [(dx, dz) for dx in range(2) for dz in range(4)]
    order = act_order.reshape(-1, HD)
    *packed, owned, most = packed_rows(packed_words, scales, order, steps)

    def few(packed, owned):
        rows = [packed[0]] + [over_head(block, *step) for block, step in zip(packed[1:], steps[1:])]
        return unpacked(depth, rows)

    def many(packed, owned):
        return from_all_rows(order, owned)

    natural = lax.cond(most[0, 0] <= CAP, few, many, packed, owned)
    near = [(0, 0, 0)] + [(dy, dx, 0) for dy in range(4) for dx in range(2) if dy or dx]
    blocks = [natural] + [over_quant(natural, *step) for step in near[1:]]
    places = near + [(dy, dx, 1) for dy, dx, _ in near]
    blocks = blocks + [over_quant(block, 0, 0, 1) for block in blocks]
    weight = None
    start = 0
    done = []
    for count in CHUNKS:
        weight, part = products(tokens, head_map, start, count, weight, places, blocks)
        done.append(z_then_x(part))
        start += count
    keys_out = jnp.concatenate([block[:, :HD] for block in done], axis=0)
    values_out = jnp.concatenate([block[:, HD:] for block in done], axis=0)
    return keys_out, values_out


def solution(mesh):
    placed = (P("quant", "head"), P("head", "quant"), P(), P(), P())
    return jax.shard_map(
        body,
        mesh=mesh,
        in_specs=placed,
        out_specs=(P("quant", "head"), P("quant", "head")),
        check_vma=False,
    )
```

```python
import functools
import jax
import jax.numpy as jnp
from jax import lax
from jax.experimental import pallas as pl
from jax.experimental.pallas import tpu as pltpu
from jax.sharding import PartitionSpec as P


KV = 8
HD = 128
G = 128
CAP = 192
TILE = 256


def over_head(value, dx, dz):
    pairs = [
        (xh * 4 + z, (xh ^ dx) * 4 + (z + dz) % 4) for xh in range(2) for z in range(4)
    ]
    return lax.ppermute(value, "head", pairs)


def over_quant(value, dy, dx, dc):
    pairs = [
        (y * 4 + x * 2 + c, (y + dy) % 4 * 4 + (x ^ dx) * 2 + (c ^ dc))
        for y in range(4)
        for x in range(2)
        for c in range(2)
    ]
    return lax.ppermute(value, "quant", pairs)


def cost(flops, moved):
    return pl.CostEstimate(flops=flops, bytes_accessed=moved, transcendentals=0)


def vmem(count):
    return [pl.BlockSpec(memory_space=pltpu.VMEM)] * count


def dequantize(words_ref, scales_ref, owned):
    words = words_ref.shape[0]
    groups = words * 4 // G
    head = lax.axis_index("head")
    quant = lax.axis_index("quant")
    scale = scales_ref[
        pl.ds(pl.multiple_of(head * groups, groups), groups),
        pl.ds(pl.multiple_of(quant * HD, HD), HD),
    ]
    spread = jnp.broadcast_to(scale[:, None, :], (groups, words // groups, HD)).reshape(
        words, HD
    )
    held = words_ref[...]
    for k in range(4):
        codes = jnp.bitwise_and(jnp.right_shift(held, 4 * k), 15)
        owned[pl.ds(k, words, stride=4), :] = (codes - 8).astype(jnp.float32) * spread


def one_hot(rows, numbers, first=0):
    at = lax.broadcasted_iota(jnp.int32, (rows, numbers.shape[1]), 0) + first
    return jnp.where(at == numbers, 1.0, 0.0).astype(jnp.bfloat16)


def in_lanes(block):
    return jnp.concatenate([block[s : s + 1, :] for s in range(block.shape[0])], axis=1)


def pack_kernel(words_ref, scales_ref, order_ref, packed_ref, owned_ref, most_ref, owned):
    dequantize(words_ref, scales_ref, owned)
    rows = owned.shape[0]
    lines = rows // HD
    parts = packed_ref.shape[0]
    head = lax.axis_index("head")
    block = owned[...].astype(jnp.bfloat16)
    owned_ref[...] = block
    fullest = jnp.zeros((lines, HD), jnp.float32)
    for source in range(parts):
        to = order_ref[source * lines : (source + 1) * lines, :] // rows
        for d in range(parts):
            count = jnp.sum(jnp.where(to == d, 1.0, 0.0))
            fullest = jnp.maximum(fullest, count)
    most_ref[...] = fullest.astype(jnp.int32)
    mine = order_ref[pl.ds(pl.multiple_of(head * lines, lines), lines), :]
    goes = mine // rows
    upto = jnp.where(
        lax.broadcasted_iota(jnp.int32, (HD, HD), 0)
        <= lax.broadcasted_iota(jnp.int32, (HD, HD), 1),
        1.0,
        0.0,
    ).astype(jnp.bfloat16)
    feature = mine % rows
    halves = jnp.concatenate(
        [in_lanes(feature // 32), in_lanes(feature % 32)], axis=0
    ).astype(jnp.float32)
    halves = jnp.concatenate([halves] + [jnp.zeros_like(halves)] * 3, axis=0)
    halves = halves.astype(jnp.bfloat16)
    for d in range(parts):
        held = jnp.where(goes == d, 1.0, 0.0)
        within = jnp.dot(held.astype(jnp.bfloat16), upto, preferred_element_type=jnp.float32)
        before = jnp.zeros((1, 1), jnp.float32)
        ranks = []
        for s in range(lines):
            ranks.append(within[s : s + 1, :] + before)
            before = before + within[s : s + 1, HD - 1 : HD]
        rank = jnp.concatenate(ranks, axis=0)
        rank = jnp.where(goes == d, rank - 1.0, -1.0).astype(jnp.int32)
        picked = one_hot(CAP, in_lanes(rank))
        packed_ref[d, :CAP, :] = jnp.dot(
            picked, block, preferred_element_type=jnp.float32
        ).astype(jnp.bfloat16)
        numbers = lax.dot_general(
            halves, picked, (((1,), (1,)), ((), ())), preferred_element_type=jnp.float32
        )
        wide = jnp.concatenate([numbers, jnp.zeros((8, 2 * HD - CAP), jnp.float32)], axis=1)
        packed_ref[d, CAP:, :] = jnp.concatenate([wide[:, :HD], wide[:, HD:]], axis=0).astype(
            jnp.bfloat16
        )


def packed_rows(words, scales, order, parts):
    rows = words.shape[0] * 4
    return pl.pallas_call(
        pack_kernel,
        out_shape=[
            jax.ShapeDtypeStruct((parts, CAP + 16, HD), jnp.bfloat16),
            jax.ShapeDtypeStruct((rows, HD), jnp.bfloat16),
            jax.ShapeDtypeStruct((8, HD), jnp.int32),
        ],
        in_specs=vmem(3),
        out_specs=vmem(3),
        scratch_shapes=[pltpu.VMEM((rows, HD), jnp.float32)],
        name="pack",
        cost_estimate=cost(1_000_000_000, 3_000_000),
    )(words, scales, order)


def halved(total, outs):
    near, far = total[: total.shape[0] // 2, :], total[total.shape[0] // 2 :, :]
    middle = HD // 2
    for side, ref in enumerate(outs):
        span = slice(side * middle, (side + 1) * middle)
        half = jnp.concatenate([near[:, span], far[:, span]], axis=1).astype(jnp.bfloat16)
        for copy in range(ref.shape[0]):
            ref[copy] = half


def unpack_kernel(packed_ref, low_ref, high_ref):
    rows = low_ref.shape[1] * 2
    total = None
    for source in range(packed_ref.shape[0]):
        tail = packed_ref[source, CAP:, :].astype(jnp.float32).astype(jnp.int32)
        number = jnp.concatenate(
            [tail[0:1, :] * 32 + tail[1:2, :], tail[8:9, :] * 32 + tail[9:10, :]], axis=1
        )
        part = jnp.dot(
            one_hot(rows, number[:, :CAP]),
            packed_ref[source, :CAP, :],
            preferred_element_type=jnp.float32,
        )
        total = part if total is None else total + part
    halved(total, (low_ref, high_ref))


def pick_kernel(order_ref, every_ref, low_ref, high_ref):
    rows = low_ref.shape[1] * 2
    lines = rows // HD
    head = lax.axis_index("head")
    total = None
    for source in range(every_ref.shape[0]):
        order = in_lanes(order_ref[source * lines : (source + 1) * lines, :])
        part = jnp.dot(
            one_hot(rows, order, head * rows),
            every_ref[source],
            preferred_element_type=jnp.float32,
        )
        total = part if total is None else total + part
    halved(total, (low_ref, high_ref))


def row_halves(kernel, name, rows, *operands):
    return pl.pallas_call(
        kernel,
        out_shape=[jax.ShapeDtypeStruct((8, rows // 2, HD), jnp.bfloat16)] * 2,
        in_specs=vmem(len(operands)),
        out_specs=vmem(2),
        name=name,
        cost_estimate=cost(1_000_000_000, 3_000_000),
    )(*operands)


def exchanged(blocks, axis, groups=None):
    return lax.all_to_all(blocks, axis, 0, 0, axis_index_groups=groups, tiled=True)


def slot_weight(map_ref, own_ref, mate_ref, relative, dz):
    head = lax.axis_index("head")
    served = map_ref[jnp.bitwise_xor(head // 4, relative) * 4 + (head % 4 + dz) % 4]
    same = served % 2 == lax.axis_index("quant") % 2
    kinds = []
    for kind in range(2):
        chip = kind * 4 + served // 2
        kinds.append(jnp.where(same, own_ref[chip], mate_ref[chip]))
    middle = HD // 2
    return jnp.concatenate(
        [
            jnp.concatenate([block[:, :middle] for block in kinds], axis=1),
            jnp.concatenate([block[:, middle:] for block in kinds], axis=1),
        ],
        axis=0,
    )


def products_kernel(plan, map_ref, x_ref, own_ref, mate_ref, *refs):
    outs, weight = refs[: len(plan)], refs[-1]
    pairs = {}
    for at, (slots, start, count) in enumerate(plan):
        for part, slot in enumerate(slots):
            pairs.setdefault((start, count), []).append((slot, outs[at], part))
    used = []
    for listed in pairs.values():
        for slot, _, _ in listed:
            if slot not in used:
                used.append(slot)
    for at, slot in enumerate(used):
        weight[:, at * HD : (at + 1) * HD] = slot_weight(map_ref, own_ref, mate_ref, *slot)
    for (start, count), listed in pairs.items():
        listed = sorted(listed, key=lambda entry: used.index(entry[0]))
        for first in range(0, len(listed), 2):
            two = listed[first : first + 2]
            left = used.index(two[0][0])
            assert used.index(two[-1][0]) == left + len(two) - 1
            for row in range(0, count, TILE):
                got = jnp.dot(
                    x_ref[start + row : start + row + TILE, :],
                    weight[:, left * HD : (left + len(two)) * HD],
                    preferred_element_type=jnp.float32,
                ).astype(jnp.bfloat16)
                for side, (_, ref, part) in enumerate(two):
                    ref[part, row : row + TILE, :] = got[:, side * HD : (side + 1) * HD]


def products(name, tokens, head_map, own, mate, plan):
    depth = tokens.shape[1]
    slots = {slot for entry in plan for slot in entry[0]}
    work = sum(len(entry[0]) * entry[2] for entry in plan)
    return pl.pallas_call(
        functools.partial(products_kernel, plan),
        out_shape=[
            jax.ShapeDtypeStruct((len(entry[0]), entry[2], HD), jnp.bfloat16) for entry in plan
        ],
        in_specs=[pl.BlockSpec(memory_space=pltpu.SMEM)] + vmem(3),
        out_specs=vmem(len(plan)),
        scratch_shapes=[pltpu.VMEM((depth, len(slots) * HD), jnp.bfloat16)],
        name=name,
        cost_estimate=cost(2 * depth * HD * work, 6_000_000),
    )(head_map, tokens, own, mate)


def added(*terms):
    total = terms[0].astype(jnp.float32)
    for term in terms[1:]:
        total = total + term.astype(jnp.float32)
    return total.astype(jnp.bfloat16)


def body(tokens, packed_words, scales, act_order, head_map):
    rows, depth = tokens.shape
    heads = lax.axis_size("head")
    order = act_order.reshape(-1, HD)
    packed, owned, most = packed_rows(packed_words, scales, order, heads)

    def few(packed, owned):
        return tuple(row_halves(unpack_kernel, "unpack", depth, exchanged(packed, "head")))

    def many(packed, owned):
        every = exchanged(jnp.broadcast_to(owned[None], (heads, *owned.shape)), "head")
        return tuple(row_halves(pick_kernel, "pick", depth, order, every))

    low, high = lax.cond(most[0, 0] <= CAP, few, many, packed, owned)
    chips = [[y * 4 + x * 2 + c for y in range(4) for x in range(2)] for c in range(2)]
    low_own = exchanged(low, "quant", chips)
    high_own = exchanged(high, "quant", chips)
    low_mate = over_quant(low_own, 0, 0, 1)
    high_mate = over_quant(high_own, 0, 0, 1)

    relay_up, relay_down = products(
        "low_relay", tokens, head_map, low_own, low_mate,
        [([(0, 2)], 0, rows), ([(1, 2)], 0, rows)],
    )
    relay_up = over_head(relay_up, 0, 1)
    relay_down = over_head(relay_down, 0, -1)
    direct_up, direct_down, turn_up, turn_down, keep, send = products(
        "low_rest", tokens, head_map, low_own, low_mate,
        [([slot], 0, rows) for slot in ((1, 1), (0, 3), (0, 1), (1, 3), (0, 0), (1, 0))],
    )
    direct_up = over_head(direct_up, 0, 1)
    direct_down = over_head(direct_down, 0, -1)
    turn_up = over_head(added(turn_up, relay_up), 0, 1)
    turn_down = over_head(added(turn_down, relay_down), 0, -1)
    across = over_head(added(send, direct_up, turn_down), 1, 0)
    low_sum = added(keep, turn_up, direct_down, across)[0]

    half = rows // 2
    (cross,) = products(
        "high_cross", tokens, head_map, high_own, high_mate,
        [([(1, dz) for dz in range(4)], 0, half)],
    )
    cross = over_head(cross, 1, 0)
    stay, near, up, down, far = products(
        "high_rest", tokens, head_map, high_own, high_mate,
        [([(0, dz) for dz in range(4)], 0, half)]
        + [([(0, dz), (1, dz)], half, half) for dz in (0, 1, 3, 2)],
    )
    up = over_head(up, 0, 1)
    down = over_head(down, 0, -1)
    far = over_head(far, 0, 2)
    joined = [added(stay[dz], cross[dz]) for dz in range(4)]
    first_up = over_head(joined[1], 0, 1)
    first_down = over_head(joined[3], 0, -1)
    first_far = over_head(joined[2], 0, 2)
    across = over_head(added(near[1], up[1], down[1], far[1]), 1, 0)
    high_first = added(joined[0], first_up, first_down, first_far)
    high_second = added(near[0], up[0], down[0], far[0], across)
    high_sum = jnp.concatenate([high_first, high_second], axis=0)
    middle = HD // 2
    keys_out = jnp.concatenate([low_sum[:, :middle], high_sum[:, :middle]], axis=1)
    values_out = jnp.concatenate([low_sum[:, middle:], high_sum[:, middle:]], axis=1)
    return keys_out, values_out


def solution(mesh):
    placed = (P("quant", "head"), P("head", "quant"), P(), P(), P())
    return jax.shard_map(
        body,
        mesh=mesh,
        in_specs=placed,
        out_specs=(P("quant", "head"), P("quant", "head")),
        check_vma=False,
    )
```

```python
import functools
import jax
import jax.numpy as jnp
from jax import lax
from jax.experimental import pallas as pl
from jax.experimental.pallas import tpu as pltpu
from jax.sharding import PartitionSpec as P


HD = 128
G = 128
CAP = 192
TILE = 256


def over_head(value, dx, dz):
    pairs = [
        (xh * 4 + z, (xh ^ dx) * 4 + (z + dz) % 4) for xh in range(2) for z in range(4)
    ]
    return lax.ppermute(value, "head", pairs)


def over_quant(value, dy, dx, dc):
    pairs = [
        (y * 4 + x * 2 + c, (y + dy) % 4 * 4 + (x ^ dx) * 2 + (c ^ dc))
        for y in range(4)
        for x in range(2)
        for c in range(2)
    ]
    return lax.ppermute(value, "quant", pairs)


def cost(flops, moved):
    return pl.CostEstimate(flops=flops, bytes_accessed=moved, transcendentals=0)


def vmem(count):
    return [pl.BlockSpec(memory_space=pltpu.VMEM)] * count


def dequantize(words_ref, scales_ref, owned):
    words = words_ref.shape[0]
    groups = words * 4 // G
    head = lax.axis_index("head")
    quant = lax.axis_index("quant")
    scale = scales_ref[
        pl.ds(pl.multiple_of(head * groups, groups), groups),
        pl.ds(pl.multiple_of(quant * HD, HD), HD),
    ]
    spread = jnp.broadcast_to(scale[:, None, :], (groups, words // groups, HD)).reshape(
        words, HD
    )
    held = words_ref[...]
    for k in range(4):
        codes = jnp.bitwise_and(jnp.right_shift(held, 4 * k), 15)
        owned[pl.ds(k, words, stride=4), :] = (codes - 8).astype(jnp.float32) * spread


def one_hot(rows, numbers, first=0):
    at = lax.broadcasted_iota(jnp.int32, (rows, numbers.shape[1]), 0) + first
    return jnp.where(at == numbers, 1.0, 0.0).astype(jnp.bfloat16)


def in_lanes(block):
    return jnp.concatenate([block[s : s + 1, :] for s in range(block.shape[0])], axis=1)


def pack_kernel(words_ref, scales_ref, order_ref, packed_ref, owned_ref, most_ref, owned):
    dequantize(words_ref, scales_ref, owned)
    rows = owned.shape[0]
    lines = rows // HD
    parts = packed_ref.shape[0]
    head = lax.axis_index("head")
    block = owned[...].astype(jnp.bfloat16)
    owned_ref[...] = block
    fullest = jnp.float32(0.0)
    for source in range(parts):
        to = order_ref[source * lines : (source + 1) * lines, :] // rows
        for d in range(parts):
            count = jnp.sum(jnp.where(to == d, 1.0, 0.0))
            fullest = jnp.maximum(fullest, count)
    most_ref[0, 0] = fullest.astype(jnp.int32)
    mine = order_ref[pl.ds(pl.multiple_of(head * lines, lines), lines), :]
    goes = mine // rows
    upto = jnp.where(
        lax.broadcasted_iota(jnp.int32, (HD, HD), 0)
        <= lax.broadcasted_iota(jnp.int32, (HD, HD), 1),
        1.0,
        0.0,
    ).astype(jnp.bfloat16)
    feature = mine % rows
    halves = jnp.concatenate(
        [in_lanes(feature // 32), in_lanes(feature % 32)], axis=0
    ).astype(jnp.float32)
    halves = jnp.concatenate([halves] + [jnp.zeros_like(halves)] * 3, axis=0)
    halves = halves.astype(jnp.bfloat16)
    for d in range(parts):
        held = jnp.where(goes == d, 1.0, 0.0)
        within = jnp.dot(held.astype(jnp.bfloat16), upto, preferred_element_type=jnp.float32)
        before = jnp.zeros((1, 1), jnp.float32)
        ranks = []
        for s in range(lines):
            ranks.append(within[s : s + 1, :] + before)
            before = before + within[s : s + 1, HD - 1 : HD]
        rank = jnp.concatenate(ranks, axis=0)
        rank = jnp.where(goes == d, rank - 1.0, -1.0).astype(jnp.int32)
        picked = one_hot(CAP, in_lanes(rank))
        packed_ref[d, :CAP, :] = jnp.dot(
            picked, block, preferred_element_type=jnp.float32
        ).astype(jnp.bfloat16)
        numbers = lax.dot_general(
            halves, picked, (((1,), (1,)), ((), ())), preferred_element_type=jnp.float32
        )
        wide = jnp.concatenate([numbers, jnp.zeros((8, 2 * HD - CAP), jnp.float32)], axis=1)
        packed_ref[d, CAP:, :] = jnp.concatenate([wide[:, :HD], wide[:, HD:]], axis=0).astype(
            jnp.bfloat16
        )


def packed_rows(words, scales, order, parts):
    rows = words.shape[0] * 4
    return pl.pallas_call(
        pack_kernel,
        out_shape=[
            jax.ShapeDtypeStruct((parts, CAP + 16, HD), jnp.bfloat16),
            jax.ShapeDtypeStruct((rows, HD), jnp.bfloat16),
            jax.ShapeDtypeStruct((1, 1), jnp.int32),
        ],
        in_specs=vmem(3),
        out_specs=vmem(2) + [pl.BlockSpec(memory_space=pltpu.SMEM)],
        scratch_shapes=[pltpu.VMEM((rows, HD), jnp.float32)],
        name="pack",
        cost_estimate=cost(1_000_000_000, 3_000_000),
    )(words, scales, order)


def halved(total, outs):
    near, far = total[: total.shape[0] // 2, :], total[total.shape[0] // 2 :, :]
    middle = HD // 2
    for side, ref in enumerate(outs):
        span = slice(side * middle, (side + 1) * middle)
        half = jnp.concatenate([near[:, span], far[:, span]], axis=1).astype(jnp.bfloat16)
        for copy in range(ref.shape[0]):
            ref[copy] = half


def unpack_kernel(packed_ref, low_ref, high_ref):
    rows = low_ref.shape[1] * 2
    total = None
    for source in range(packed_ref.shape[0]):
        tail = packed_ref[source, CAP:, :].astype(jnp.float32).astype(jnp.int32)
        number = jnp.concatenate(
            [tail[0:1, :] * 32 + tail[1:2, :], tail[8:9, :] * 32 + tail[9:10, :]], axis=1
        )
        part = jnp.dot(
            one_hot(rows, number[:, :CAP]),
            packed_ref[source, :CAP, :],
            preferred_element_type=jnp.float32,
        )
        total = part if total is None else total + part
    halved(total, (low_ref, high_ref))


def pick_kernel(order_ref, every_ref, low_ref, high_ref):
    rows = low_ref.shape[1] * 2
    lines = rows // HD
    head = lax.axis_index("head")
    total = None
    for source in range(every_ref.shape[0]):
        order = in_lanes(order_ref[source * lines : (source + 1) * lines, :])
        part = jnp.dot(
            one_hot(rows, order, head * rows),
            every_ref[source],
            preferred_element_type=jnp.float32,
        )
        total = part if total is None else total + part
    halved(total, (low_ref, high_ref))


def row_halves(kernel, rows, *operands):
    return pl.pallas_call(
        kernel,
        out_shape=[jax.ShapeDtypeStruct((8, rows // 2, HD), jnp.bfloat16)] * 2,
        in_specs=vmem(len(operands)),
        out_specs=vmem(2),
        cost_estimate=cost(1_000_000_000, 3_000_000),
    )(*operands)


def exchanged(blocks, axis, groups=None):
    return lax.all_to_all(blocks, axis, 0, 0, axis_index_groups=groups, tiled=True)


def slot_weight(map_ref, own_ref, mate_ref, relative, dz):
    head = lax.axis_index("head")
    served = map_ref[jnp.bitwise_xor(head // 4, relative) * 4 + (head % 4 + dz) % 4]
    same = served % 2 == lax.axis_index("quant") % 2
    kinds = []
    for kind in range(2):
        chip = kind * 4 + served // 2
        kinds.append(jnp.where(same, own_ref[chip], mate_ref[chip]))
    middle = HD // 2
    return jnp.concatenate(
        [
            jnp.concatenate([block[:, :middle] for block in kinds], axis=1),
            jnp.concatenate([block[:, middle:] for block in kinds], axis=1),
        ],
        axis=0,
    )


def products_kernel(plan, map_ref, x_ref, own_ref, mate_ref, *refs):
    outs, weight = refs[: len(plan)], refs[-1]
    listed = [(slot, outs[at], part) for at, slots in enumerate(plan) for part, slot in enumerate(slots)]

    @pl.when(pl.program_id(0) == 0)
    def _():
        for at, (slot, _, _) in enumerate(listed):
            weight[:, at * HD : (at + 1) * HD] = slot_weight(map_ref, own_ref, mate_ref, *slot)

    for first in range(0, len(listed), 2):
        two = listed[first : first + 2]
        got = jnp.dot(
            x_ref[...],
            weight[:, first * HD : (first + len(two)) * HD],
            preferred_element_type=jnp.float32,
        ).astype(jnp.bfloat16)
        for side, (_, ref, part) in enumerate(two):
            ref[part] = got[:, side * HD : (side + 1) * HD]


def products(tokens, head_map, own, mate, start, rows, plan):
    depth = tokens.shape[1]
    slots = sum(len(entry) for entry in plan)
    whole = pl.BlockSpec(memory_space=pltpu.VMEM)
    return pl.pallas_call(
        functools.partial(products_kernel, plan),
        grid=(rows // TILE,),
        out_shape=[jax.ShapeDtypeStruct((len(entry), rows, HD), jnp.bfloat16) for entry in plan],
        in_specs=[
            pl.BlockSpec(memory_space=pltpu.SMEM),
            pl.BlockSpec((TILE, depth), lambda i: (start // TILE + i, 0)),
            whole,
            whole,
        ],
        out_specs=[pl.BlockSpec((len(entry), TILE, HD), lambda i: (0, i, 0)) for entry in plan],
        scratch_shapes=[pltpu.VMEM((depth, slots * HD), jnp.bfloat16)],
        cost_estimate=cost(2 * depth * HD * slots * rows, 6_000_000),
    )(head_map, tokens, own, mate)


def added(*terms):
    total = terms[0].astype(jnp.float32)
    for term in terms[1:]:
        total = total + term.astype(jnp.float32)
    return total.astype(jnp.bfloat16)


def body(tokens, packed_words, scales, act_order, head_map):
    rows, depth = tokens.shape
    heads = lax.axis_size("head")
    order = act_order.reshape(-1, HD)
    packed, owned, most = packed_rows(packed_words, scales, order, heads)

    def few(packed, owned):
        return tuple(row_halves(unpack_kernel, depth, exchanged(packed, "head")))

    def many(packed, owned):
        every = exchanged(jnp.broadcast_to(owned[None], (heads, *owned.shape)), "head")
        return tuple(row_halves(pick_kernel, depth, order, every))

    low, high = lax.cond(most[0, 0] <= CAP, few, many, packed, owned)
    chips = [[y * 4 + x * 2 + c for y in range(4) for x in range(2)] for c in range(2)]
    low_own = exchanged(low, "quant", chips)
    high_own = exchanged(high, "quant", chips)
    low_mate = over_quant(low_own, 0, 0, 1)
    high_mate = over_quant(high_own, 0, 0, 1)

    relay_up, relay_down = products(
        tokens, head_map, low_own, low_mate, 0, rows, [[(0, 2)], [(1, 2)]]
    )
    relay_up = over_head(relay_up, 0, 1)
    relay_down = over_head(relay_down, 0, -1)
    direct_up, direct_down, turn_up, turn_down, keep, send = products(
        tokens, head_map, low_own, low_mate, 0, rows,
        [[slot] for slot in ((1, 1), (0, 3), (0, 1), (1, 3), (0, 0), (1, 0))],
    )
    direct_up = over_head(direct_up, 0, 1)
    direct_down = over_head(direct_down, 0, -1)
    turn_up = over_head(added(turn_up, relay_up), 0, 1)
    turn_down = over_head(added(turn_down, relay_down), 0, -1)
    across = over_head(added(send, direct_up, turn_down), 1, 0)
    low_sum = added(keep, turn_up, direct_down, across)[0]

    half = rows // 2
    (cross,) = products(
        tokens, head_map, high_own, high_mate, 0, half, [[(1, dz) for dz in range(4)]]
    )
    cross = over_head(cross, 1, 0)
    up, down, far, near = products(
        tokens, head_map, high_own, high_mate, half, half,
        [[(0, dz), (1, dz)] for dz in (1, 3, 2, 0)],
    )
    up = over_head(up, 0, 1)
    down = over_head(down, 0, -1)
    far = over_head(far, 0, 2)
    (stay,) = products(
        tokens, head_map, high_own, high_mate, 0, half, [[(0, dz) for dz in range(4)]]
    )
    joined = [added(stay[dz], cross[dz]) for dz in range(4)]
    first_up = over_head(joined[1], 0, 1)
    first_down = over_head(joined[3], 0, -1)
    first_far = over_head(joined[2], 0, 2)
    across = over_head(added(near[1], up[1], down[1], far[1]), 1, 0)
    high_first = added(joined[0], first_up, first_down, first_far)
    high_second = added(near[0], up[0], down[0], far[0], across)
    high_sum = jnp.concatenate([high_first, high_second], axis=0)
    middle = HD // 2
    keys_out = jnp.concatenate([low_sum[:, :middle], high_sum[:, :middle]], axis=1)
    values_out = jnp.concatenate([low_sum[:, middle:], high_sum[:, middle:]], axis=1)
    return keys_out, values_out


def solution(mesh):
    placed = (P("quant", "head"), P("head", "quant"), P(), P(), P())
    return jax.shard_map(
        body,
        mesh=mesh,
        in_specs=placed,
        out_specs=(P("quant", "head"), P("quant", "head")),
        check_vma=False,
    )
```

```python
import functools
import jax
import jax.numpy as jnp
from jax import lax
from jax.experimental import pallas as pl
from jax.experimental.pallas import tpu as pltpu
from jax.sharding import PartitionSpec as P


HD = 128
G = 128
CAP = 192
TILE = 256
ROOMY = pltpu.CompilerParams(vmem_limit_bytes=20 * 1024 * 1024)


def over_head(value, dx, dz):
    pairs = [
        (xh * 4 + z, (xh ^ dx) * 4 + (z + dz) % 4) for xh in range(2) for z in range(4)
    ]
    return lax.ppermute(value, "head", pairs)


def over_quant(value, dy, dx, dc):
    pairs = [
        (y * 4 + x * 2 + c, (y + dy) % 4 * 4 + (x ^ dx) * 2 + (c ^ dc))
        for y in range(4)
        for x in range(2)
        for c in range(2)
    ]
    return lax.ppermute(value, "quant", pairs)


def cost(flops, moved):
    return pl.CostEstimate(flops=flops, bytes_accessed=moved, transcendentals=0)


def vmem(count):
    return [pl.BlockSpec(memory_space=pltpu.VMEM)] * count


def dequantize(words_ref, scales_ref, owned):
    words = words_ref.shape[0]
    groups = words * 4 // G
    head = lax.axis_index("head")
    quant = lax.axis_index("quant")
    scale = scales_ref[
        pl.ds(pl.multiple_of(head * groups, groups), groups),
        pl.ds(pl.multiple_of(quant * HD, HD), HD),
    ]
    spread = jnp.broadcast_to(scale[:, None, :], (groups, words // groups, HD)).reshape(
        words, HD
    )
    held = words_ref[...]
    for k in range(4):
        codes = jnp.bitwise_and(jnp.right_shift(held, 4 * k), 15)
        owned[pl.ds(k, words, stride=4), :] = (codes - 8).astype(jnp.float32) * spread


def one_hot(rows, numbers, first=0):
    at = lax.broadcasted_iota(jnp.int32, (rows, numbers.shape[1]), 0) + first
    return jnp.where(at == numbers, 1.0, 0.0).astype(jnp.bfloat16)


def in_lanes(block):
    return jnp.concatenate([block[s : s + 1, :] for s in range(block.shape[0])], axis=1)


def pack_kernel(words_ref, scales_ref, order_ref, packed_ref, owned_ref, most_ref, owned):
    dequantize(words_ref, scales_ref, owned)
    rows = owned.shape[0]
    lines = rows // HD
    parts = packed_ref.shape[0]
    head = lax.axis_index("head")
    block = owned[...].astype(jnp.bfloat16)
    owned_ref[...] = block
    fullest = jnp.float32(0.0)
    for source in range(parts):
        to = order_ref[source * lines : (source + 1) * lines, :] // rows
        for d in range(parts):
            count = jnp.sum(jnp.where(to == d, 1.0, 0.0))
            fullest = jnp.maximum(fullest, count)
    most_ref[0, 0] = fullest.astype(jnp.int32)
    mine = order_ref[pl.ds(pl.multiple_of(head * lines, lines), lines), :]
    goes = mine // rows
    upto = jnp.where(
        lax.broadcasted_iota(jnp.int32, (HD, HD), 0)
        <= lax.broadcasted_iota(jnp.int32, (HD, HD), 1),
        1.0,
        0.0,
    ).astype(jnp.bfloat16)
    feature = mine % rows
    halves = jnp.concatenate(
        [in_lanes(feature // 32), in_lanes(feature % 32)], axis=0
    ).astype(jnp.float32)
    halves = jnp.concatenate([halves] + [jnp.zeros_like(halves)] * 3, axis=0)
    halves = halves.astype(jnp.bfloat16)
    for d in range(parts):
        held = jnp.where(goes == d, 1.0, 0.0)
        within = jnp.dot(held.astype(jnp.bfloat16), upto, preferred_element_type=jnp.float32)
        before = jnp.zeros((1, 1), jnp.float32)
        ranks = []
        for s in range(lines):
            ranks.append(within[s : s + 1, :] + before)
            before = before + within[s : s + 1, HD - 1 : HD]
        rank = jnp.concatenate(ranks, axis=0)
        rank = jnp.where(goes == d, rank - 1.0, -1.0).astype(jnp.int32)
        picked = one_hot(CAP, in_lanes(rank))
        packed_ref[d, :CAP, :] = jnp.dot(
            picked, block, preferred_element_type=jnp.float32
        ).astype(jnp.bfloat16)
        numbers = lax.dot_general(
            halves, picked, (((1,), (1,)), ((), ())), preferred_element_type=jnp.float32
        )
        wide = jnp.concatenate([numbers, jnp.zeros((8, 2 * HD - CAP), jnp.float32)], axis=1)
        packed_ref[d, CAP:, :] = jnp.concatenate([wide[:, :HD], wide[:, HD:]], axis=0).astype(
            jnp.bfloat16
        )


def packed_rows(words, scales, order, parts):
    rows = words.shape[0] * 4
    return pl.pallas_call(
        pack_kernel,
        out_shape=[
            jax.ShapeDtypeStruct((parts, CAP + 16, HD), jnp.bfloat16),
            jax.ShapeDtypeStruct((rows, HD), jnp.bfloat16),
            jax.ShapeDtypeStruct((1, 1), jnp.int32),
        ],
        in_specs=vmem(3),
        out_specs=vmem(2) + [pl.BlockSpec(memory_space=pltpu.SMEM)],
        scratch_shapes=[pltpu.VMEM((rows, HD), jnp.float32)],
        name="pack",
        cost_estimate=cost(1_000_000_000, 3_000_000),
        compiler_params=ROOMY,
    )(words, scales, order)


def halved(total, outs):
    near, far = total[: total.shape[0] // 2, :], total[total.shape[0] // 2 :, :]
    middle = HD // 2
    for side, ref in enumerate(outs):
        span = slice(side * middle, (side + 1) * middle)
        half = jnp.concatenate([near[:, span], far[:, span]], axis=1).astype(jnp.bfloat16)
        for copy in range(ref.shape[0]):
            ref[copy] = half


def unpack_kernel(packed_ref, low_ref, high_ref):
    rows = low_ref.shape[1] * 2
    total = None
    for source in range(packed_ref.shape[0]):
        tail = packed_ref[source, CAP:, :].astype(jnp.float32).astype(jnp.int32)
        number = jnp.concatenate(
            [tail[0:1, :] * 32 + tail[1:2, :], tail[8:9, :] * 32 + tail[9:10, :]], axis=1
        )
        part = jnp.dot(
            one_hot(rows, number[:, :CAP]),
            packed_ref[source, :CAP, :],
            preferred_element_type=jnp.float32,
        )
        total = part if total is None else total + part
    halved(total, (low_ref, high_ref))


def pick_kernel(order_ref, every_ref, low_ref, high_ref):
    rows = low_ref.shape[1] * 2
    lines = rows // HD
    head = lax.axis_index("head")
    total = None
    for source in range(every_ref.shape[0]):
        order = in_lanes(order_ref[source * lines : (source + 1) * lines, :])
        part = jnp.dot(
            one_hot(rows, order, head * rows),
            every_ref[source],
            preferred_element_type=jnp.float32,
        )
        total = part if total is None else total + part
    halved(total, (low_ref, high_ref))


def row_halves(kernel, rows, *operands):
    return pl.pallas_call(
        kernel,
        out_shape=[jax.ShapeDtypeStruct((8, rows // 2, HD), jnp.bfloat16)] * 2,
        in_specs=vmem(len(operands)),
        out_specs=vmem(2),
        cost_estimate=cost(1_000_000_000, 3_000_000),
        compiler_params=ROOMY,
    )(*operands)


def exchanged(blocks, axis, groups=None):
    return lax.all_to_all(blocks, axis, 0, 0, axis_index_groups=groups, tiled=True)


def slot_weight(map_ref, own_ref, mate_ref, relative, dz):
    head = lax.axis_index("head")
    served = map_ref[jnp.bitwise_xor(head // 4, relative) * 4 + (head % 4 + dz) % 4]
    same = served % 2 == lax.axis_index("quant") % 2
    kinds = []
    for kind in range(2):
        chip = kind * 4 + served // 2
        kinds.append(jnp.where(same, own_ref[chip], mate_ref[chip]))
    middle = HD // 2
    return jnp.concatenate(
        [
            jnp.concatenate([block[:, :middle] for block in kinds], axis=1),
            jnp.concatenate([block[:, middle:] for block in kinds], axis=1),
        ],
        axis=0,
    )


def products_kernel(plan, start, map_ref, x_ref, own_ref, mate_ref, *refs):
    outs, weight = refs[: len(plan)], refs[-1]
    listed = [(slot, outs[at], part) for at, slots in enumerate(plan) for part, slot in enumerate(slots)]
    rows = outs[0].shape[1]
    for first in range(0, len(listed), 2):
        two = listed[first : first + 2]
        for side, (slot, _, _) in enumerate(two):
            weight[:, side * HD : (side + 1) * HD] = slot_weight(map_ref, own_ref, mate_ref, *slot)
        for row in range(0, rows, TILE):
            got = jnp.dot(
                x_ref[start + row : start + row + TILE, :],
                weight[...],
                preferred_element_type=jnp.float32,
            ).astype(jnp.bfloat16)
            for side, (_, ref, part) in enumerate(two):
                ref[part, row : row + TILE, :] = got[:, side * HD : (side + 1) * HD]


def products(tokens, head_map, own, mate, start, rows, plan):
    depth = tokens.shape[1]
    slots = sum(len(entry) for entry in plan)
    return pl.pallas_call(
        functools.partial(products_kernel, plan, start),
        out_shape=[jax.ShapeDtypeStruct((len(entry), rows, HD), jnp.bfloat16) for entry in plan],
        in_specs=[pl.BlockSpec(memory_space=pltpu.SMEM)] + vmem(3),
        out_specs=vmem(len(plan)),
        scratch_shapes=[pltpu.VMEM((depth, 2 * HD), jnp.bfloat16)],
        cost_estimate=cost(2 * depth * HD * slots * rows, 6_000_000),
        compiler_params=ROOMY,
    )(head_map, tokens, own, mate)


def added(*terms):
    total = terms[0].astype(jnp.float32)
    for term in terms[1:]:
        total = total + term.astype(jnp.float32)
    return total.astype(jnp.bfloat16)


def body(tokens, packed_words, scales, act_order, head_map):
    rows, depth = tokens.shape
    heads = lax.axis_size("head")
    order = act_order.reshape(-1, HD)
    packed, owned, most = packed_rows(packed_words, scales, order, heads)

    def few(packed, owned):
        return tuple(row_halves(unpack_kernel, depth, exchanged(packed, "head")))

    def many(packed, owned):
        every = exchanged(jnp.broadcast_to(owned[None], (heads, *owned.shape)), "head")
        return tuple(row_halves(pick_kernel, depth, order, every))

    low, high = lax.cond(most[0, 0] <= CAP, few, many, packed, owned)
    chips = [[y * 4 + x * 2 + c for y in range(4) for x in range(2)] for c in range(2)]
    low_own = exchanged(low, "quant", chips)
    high_own = exchanged(high, "quant", chips)
    low_mate = over_quant(low_own, 0, 0, 1)
    high_mate = over_quant(high_own, 0, 0, 1)

    relay_up, relay_down = products(
        tokens, head_map, low_own, low_mate, 0, rows, [[(0, 2)], [(1, 2)]]
    )
    relay_up = over_head(relay_up, 0, 1)
    relay_down = over_head(relay_down, 0, -1)
    direct_up, direct_down, turn_up, turn_down, keep, send = products(
        tokens, head_map, low_own, low_mate, 0, rows,
        [[slot] for slot in ((1, 1), (0, 3), (0, 1), (1, 3), (0, 0), (1, 0))],
    )
    direct_up = over_head(direct_up, 0, 1)
    direct_down = over_head(direct_down, 0, -1)
    turn_up = over_head(added(turn_up, relay_up), 0, 1)
    turn_down = over_head(added(turn_down, relay_down), 0, -1)
    across = over_head(added(send, direct_up, turn_down), 1, 0)
    low_sum = added(keep, turn_up, direct_down, across)[0]

    half = rows // 2
    (cross,) = products(
        tokens, head_map, high_own, high_mate, 0, half, [[(1, dz) for dz in range(4)]]
    )
    cross = over_head(cross, 1, 0)
    up, down, far, near = products(
        tokens, head_map, high_own, high_mate, half, half,
        [[(0, dz), (1, dz)] for dz in (1, 3, 2, 0)],
    )
    up = over_head(up, 0, 1)
    down = over_head(down, 0, -1)
    far = over_head(far, 0, 2)
    (stay,) = products(
        tokens, head_map, high_own, high_mate, 0, half, [[(0, dz) for dz in range(4)]]
    )
    joined = [added(stay[dz], cross[dz]) for dz in range(4)]
    first_up = over_head(joined[1], 0, 1)
    first_down = over_head(joined[3], 0, -1)
    first_far = over_head(joined[2], 0, 2)
    across = over_head(added(near[1], up[1], down[1], far[1]), 1, 0)
    high_first = added(joined[0], first_up, first_down, first_far)
    high_second = added(near[0], up[0], down[0], far[0], across)
    high_sum = jnp.concatenate([high_first, high_second], axis=0)
    middle = HD // 2
    keys_out = jnp.concatenate([low_sum[:, :middle], high_sum[:, :middle]], axis=1)
    values_out = jnp.concatenate([low_sum[:, middle:], high_sum[:, middle:]], axis=1)
    return keys_out, values_out


def solution(mesh):
    placed = (P("quant", "head"), P("head", "quant"), P(), P(), P())
    return jax.shard_map(
        body,
        mesh=mesh,
        in_specs=placed,
        out_specs=(P("quant", "head"), P("quant", "head")),
        check_vma=False,
    )
```
